256 devices in a mesh: wide: 64 (over x, z_hi, y), narrow: 4 (over z_lo, core).
Axes of the slice: x: 4, y: 4, z: 8 (z_hi: 4, z_lo: 2; z = z_hi * 2 + z_lo), core: 2. Of those that a mesh axis runs over, the one named last changes fastest.
Arguments:
- coefficients: bfloat16 [512, 2, 256, 512], P(('wide', 'narrow')), may hold values from -6 to 6
- col_weights: bfloat16 [2, 512, 2, 256, 512], P(None, ('wide', 'narrow')), may hold values from -0.1875 to 0.1875
- row_weights: bfloat16 [2, 512, 2, 256, 512], P(None, 'wide'), may hold values from -0.1875 to 0.1875
Outputs:
- applied: bfloat16 [512, 2, 256, 512], P('wide', None, None, 'narrow')
The draws below stay inside these ranges and needn't reach their ends.
All inputs are finite; a program needn't handle non-finite values.
Results may differ from the reference program's by a relative error of at most 0.0064.
Values may be sent and summed in bfloat16 or wider, within the bound.
A program may use at most 64 MiB of HBM per device.

```python
import jax
import jax.numpy as jnp
from jax import lax

R = 256
NRHS = 512
NODE_DEV = 2
NODES = 512
N_NARROW = 4


def steps_of(key, dims, split, smallest, high):
    gain = 1.0
    for dim, blocks in split:
        heights = jax.random.uniform(jax.random.fold_in(jax.random.fold_in(key, 6), dim), (blocks,), jnp.float32, smallest / len(split), high / len(split))
        gain = gain * jnp.repeat(jnp.exp(heights), dims[dim] // blocks).reshape((-1,) + (1,) * (len(dims) - 1 - dim))
    return gain


def centred(rng, shape, scale, most, pieces=(), held_as=jnp.bfloat16):
    values = jax.random.normal(rng, shape, jnp.float32) * scale
    if len(pieces) > 0:
        values = steps_of(rng, shape, pieces, -0.22, 0.18) * values
    return jnp.clip(values, min=-most, max=most).astype(held_as)


def setup_inputs(seed: int = 0) -> dict:
    key_list = jax.random.split(jax.random.key(seed), 4)
    return {
        "coefficients": centred(key_list[0], (NODES, 2, R, NRHS), 1.0, 6.0, ((0, 256),)),
        "col_weights": centred(key_list[1], (2, NODES, 2, R, 2 * R), (4 * R) ** -0.5, 0.1875, ((1, 256),)),
        "row_weights": centred(key_list[2], (2, NODES, 2, R, 2 * R), (4 * R) ** -0.5, 0.1875, ((1, 64),)),
    }


def apply_level(coef, weights, distance):
    count = coef.shape[-1]
    groups = coef.shape[0] // (2 * distance)
    blocks = coef.reshape(groups, 2, distance, 2, R, count).astype(jnp.float32)
    stacked = jnp.concatenate([blocks[:, 0], blocks[:, 1]], axis=3)
    merged = jnp.concatenate([stacked[:, :, 0], stacked[:, :, 1]], axis=-1)
    mats = weights.reshape(groups, 2, distance, 2, R, 2 * R).astype(jnp.float32)
    first = jnp.einsum('ghdab,gdbn->ghdan', mats[:, :, :, 0], merged, precision=lax.Precision.HIGHEST)
    second = jnp.einsum('ghdab,gdbn->ghdan', mats[:, :, :, 1], merged, precision=lax.Precision.HIGHEST)
    real = first[..., :count] - second[..., count:]
    imag = first[..., count:] + second[..., :count]
    result = jnp.stack([real, imag], axis=3)
    return result.reshape(coef.shape[0], 2, R, count).astype(jnp.bfloat16)


def reference(coefficients, col_weights, row_weights):
    group = NODE_DEV * N_NARROW
    state = apply_level(coefficients, col_weights[0], group)
    state = apply_level(state, col_weights[1], 2 * group)
    state = apply_level(state, row_weights[0], NODES // 4)
    state = apply_level(state, row_weights[1], NODES // 2)
    return state
```

```python
import functools

import jax
import jax.numpy as jnp
from jax import lax
from jax.experimental import pallas as pl
from jax.experimental.pallas import tpu as pltpu
from jax.sharding import PartitionSpec as P

MESH = pl.DeviceIdType.MESH
TURNS = (2, 3, 1, 0)
AHEAD = 2


def turned(index, turn):
    if turn == 0:
        return index
    if turn == 1:
        return index + 1 - 2 * (index % 2)
    if turn == 2:
        return index + 2 - 4 * (index // 2)
    return 3 - index


def multiply(weights, block, store):
    merged = block[...].reshape(weights.shape[2], block.shape[2])
    half = merged.shape[1] // 2
    first = jnp.dot(weights[0], merged, preferred_element_type=jnp.float32)
    second = jnp.dot(weights[1], merged, preferred_element_type=jnp.float32)
    real = first[:, :half] - second[:, half:]
    imag = first[:, half:] + second[:, :half]
    store(real.astype(jnp.bfloat16), imag.astype(jnp.bfloat16))


def events(chunks, moved):
    timed = []
    for c in range(chunks):
        one = 2 * c + 0.6 if c else 1.6
        two = 3.6 + 2 * c
        if c == chunks - 1:
            two -= 1
        relay = two + 1.7 if c < moved - 2 else two + 0.6
        three = (relay if c < moved else two) + 1.7
        four = three + 2
        timed += [(one, 1, c), (two, 2, c), (three, 4, c), (four, 5, c)]
        if c < moved:
            timed.append((relay, 3, c))
    return [(stage, c) for _, stage, c in sorted(timed)]


def kernel(wide_bits, coef, colw, roww, out, x1, x2, x3, x4, stage, done, cw, rw,
           coef_sem, cw_sem, rw_sem, out_sem, send, recv):
    w = lax.axis_index("wide")
    n = lax.axis_index("narrow")
    nodes = coef.shape[0]
    turns = len(TURNS)
    chunks = nodes * turns
    moved = chunks - nodes
    cols = x1.shape[3] // 2

    def bit(i):
        return (w // 2**i) % 2

    def swapped(i):
        return w + 2**i - 2 ** (i + 1) * bit(i)

    levels = (0, 1, wide_bits - 2, wide_bits - 1)
    b1, b2, b3, b4 = (bit(i) for i in levels)
    partner = [(swapped(i), n) for i in levels]

    def turn_of(c):
        return TURNS[c // nodes]

    coef_copies, cw_copies, rw_copies = [], {}, {}
    for c in range(chunks):
        column = pl.multiple_of(turned(n, turn_of(c)) * cols, cols)
        coef_copies.append([
            pltpu.make_async_copy(
                coef.at[c % nodes, plane, :, pl.ds(column, cols)],
                x1.at[c, b1, :, plane * cols:(plane + 1) * cols],
                coef_sem.at[c, plane],
            )
            for plane in range(2)
        ])
    for level in range(2):
        for k in range(nodes):
            cw_copies[level, k] = pltpu.make_async_copy(colw.at[level, k], cw.at[level, k], cw_sem.at[level, k])
        for c in range(chunks):
            node = turned(n, turn_of(c)) * nodes + c % nodes
            rw_copies[level, c] = pltpu.make_async_copy(roww.at[level, node], rw.at[level, c], rw_sem.at[level, c])

    for pair in coef_copies[:AHEAD]:
        for copy in pair:
            copy.start()
    barrier = pltpu.get_barrier_semaphore()
    greeted = partner + [(w, turned(n, turn)) for turn in range(1, turns)]
    for device in greeted:
        pl.semaphore_signal(barrier, inc=1, device_id=device, device_id_type=MESH)
    for k in range(nodes):
        cw_copies[0, k].start()
    for pair in coef_copies[AHEAD:]:
        for copy in pair:
            copy.start()
    for k in range(nodes):
        cw_copies[1, k].start()
    for c in range(chunks):
        for level in range(2):
            rw_copies[level, c].start()
    pl.semaphore_wait(barrier, len(greeted))

    def exchange(stage_index, c, src, dst, device):
        return pltpu.make_async_remote_copy(
            src_ref=src,
            dst_ref=dst,
            send_sem=send.at[stage_index, c],
            recv_sem=recv.at[stage_index, c],
            device_id=device,
            device_id_type=MESH,
        )

    ex1 = [exchange(0, c, x1.at[c, b1], x1.at[c, b1], partner[0]) for c in range(chunks)]
    ex2 = [exchange(1, c, x2.at[c, b2], x2.at[c, b2], partner[1]) for c in range(chunks)]
    relay = [
        exchange(2, c, stage.at[c], x3.at[c, b3], (w, turned(n, turn_of(c)))) for c in range(moved)
    ]
    ex3 = [exchange(3, c, x3.at[c, b3], x3.at[c, b3], partner[2]) for c in range(chunks)]
    ex4 = [exchange(4, c, x4.at[c, b4], x4.at[c, b4], partner[3]) for c in range(chunks)]
    out_copies = []

    def begin(c):
        for copy in coef_copies[c]:
            copy.wait()
        ex1[c].start()

    def into(ref, *index):
        def store(real, imag):
            ref[(*index, slice(None), slice(0, cols))] = real
            ref[(*index, slice(None), slice(cols, 2 * cols))] = imag
        return store

    for c in range(AHEAD):
        begin(c)
    for step, c in events(chunks, moved):
        k = c % nodes
        if step == 1:
            if c + AHEAD < chunks:
                begin(c + AHEAD)
            if c < nodes:
                cw_copies[0, k].wait()
            ex1[c].wait_recv()
            multiply(cw.at[0, k], x1.at[c], into(x2, c, b2))
            ex2[c].start()
        elif step == 2:
            if c < nodes:
                cw_copies[1, k].wait()
            ex2[c].wait_recv()
            if c < moved:
                multiply(cw.at[1, k], x2.at[c], into(stage, c))
                relay[c].start()
            else:
                multiply(cw.at[1, k], x2.at[c], into(x3, c, b3))
                ex3[c].start()
        elif step == 3:
            relay[c].wait_recv()
            ex3[c].start()
        elif step == 4:
            rw_copies[0, c].wait()
            ex3[c].wait_recv()
            multiply(rw.at[0, c], x3.at[c], into(x4, c, b4))
            ex4[c].start()
        else:
            rw_copies[1, c].wait()
            ex4[c].wait_recv()
            multiply(rw.at[1, c], x4.at[c], into(done, c))
            node = turned(n, turn_of(c)) * nodes + k
            for plane in range(2):
                copy = pltpu.make_async_copy(
                    done.at[c, :, plane * cols:(plane + 1) * cols], out.at[node, plane], out_sem.at[c, plane]
                )
                copy.start()
                out_copies.append(copy)
    for copy in ex1 + ex2 + relay + ex3 + ex4:
        copy.wait_send()
    for copy in out_copies:
        copy.wait()


def solution(mesh):
    narrow = mesh.shape["narrow"]
    wide_bits = mesh.shape["wide"].bit_length() - 1

    def per_device(coefficients, col_weights, row_weights):
        nodes, _, rank, count = coefficients.shape
        cols = count // narrow
        chunks = nodes * narrow
        block = (chunks, 2, rank, 2 * cols)
        dtype = jnp.bfloat16
        flops = 4 * chunks * 2 * 2 * rank * 2 * rank * 2 * cols
        moved = 2 * (coefficients.size * 2 + col_weights.size + row_weights.size)
        dma = pltpu.SemaphoreType.DMA
        return pl.pallas_call(
            functools.partial(kernel, wide_bits),
            out_shape=jax.ShapeDtypeStruct((chunks, 2, rank, cols), dtype),
            in_specs=[pl.BlockSpec(memory_space=pl.ANY)] * 3,
            out_specs=pl.BlockSpec(memory_space=pl.ANY),
            scratch_shapes=[
                pltpu.VMEM(block, dtype),
                pltpu.VMEM(block, dtype),
                pltpu.VMEM(block, dtype),
                pltpu.VMEM(block, dtype),
                pltpu.VMEM((chunks - nodes, rank, 2 * cols), dtype),
                pltpu.VMEM((chunks, rank, 2 * cols), dtype),
                pltpu.VMEM((2, nodes, 2, rank, 2 * rank), dtype),
                pltpu.VMEM((2, chunks, 2, rank, 2 * rank), dtype),
                dma((chunks, 2)),
                dma((2, nodes)),
                dma((2, chunks)),
                dma((chunks, 2)),
                dma((5, chunks)),
                dma((5, chunks)),
            ],
            compiler_params=pltpu.CompilerParams(
                collective_id=0, has_side_effects=True, vmem_limit_bytes=60 * 2**20
            ),
            cost_estimate=pl.CostEstimate(flops=flops, bytes_accessed=moved, transcendentals=0),
        )(coefficients, col_weights, row_weights)

    return jax.shard_map(
        per_device,
        mesh=mesh,
        in_specs=(
            P(("wide", "narrow"), None, None, None),
            P(None, ("wide", "narrow"), None, None, None),
            P(None, "wide", None, None, None),
        ),
        out_specs=P("wide", None, None, "narrow"),
        check_vma=False,
    )
```

```python
import functools

import jax
import jax.numpy as jnp
from jax import lax
from jax.experimental import pallas as pl
from jax.experimental.pallas import tpu as pltpu
from jax.sharding import PartitionSpec as P

MESH = pl.DeviceIdType.MESH
TURNS = (0, 3, 2, 1)
AHEAD = 1
PARTS = 2
LAGS = (2.05, 1.6, 2.6)


def turned(index, turn):
    if turn == 0:
        return index
    if turn == 1:
        return index + 1 - 2 * (index % 2)
    if turn == 2:
        return index + 2 - 4 * (index // 2)
    return 3 - index


def halves(width):
    return lax.broadcasted_iota(jnp.int32, (1, width), 1) < width // 2


def crossed(array):
    return pltpu.roll(array, array.shape[1] // 2, 1)


def product(weights, block):
    merged = block[...].reshape(weights.shape[2], block.shape[2])
    first = jnp.dot(weights[0], merged, preferred_element_type=jnp.float32)
    second = crossed(jnp.dot(weights[1], merged, preferred_element_type=jnp.float32))
    return jnp.where(halves(merged.shape[1]), first - second, first + second)


def traded(a, b):
    left = halves(a.shape[1])
    return jnp.where(left, a, crossed(b)), jnp.where(left, crossed(a), b)


def events(chunks):
    expected = (0, LAGS[0], LAGS[0] + LAGS[1], sum(LAGS))
    return [(level, c) for _, level, c in sorted((c + late, level, c) for c in range(chunks) for level, late in enumerate(expected))]


def kernel(wide_bits, coef, colw, roww, out, blocks, x1, x2, x3, x4, stage, done, cw, rw,
           coef_sem, cw_sem, rw_sem, out_sem, send, recv):
    w = lax.axis_index("wide")
    n = lax.axis_index("narrow")
    nodes = coef.shape[0]
    turns = len(TURNS)
    pairs = nodes * turns
    chunks = pairs * PARTS
    cols = blocks.shape[3]

    def bit(i):
        return (w // 2**i) % 2

    def swapped(i):
        return w + 2**i - 2 ** (i + 1) * bit(i)

    levels = (0, 1, wide_bits - 2, wide_bits - 1)
    b1, b2, b3, b4 = (bit(i) for i in levels)
    partner = [(swapped(i), n) for i in levels]

    def turn_of(pair):
        return TURNS[pair // nodes]

    coef_copies, cw_copies, rw_copies = [], {}, {}
    for pair in range(pairs):
        column = pl.multiple_of(turned(n, turn_of(pair)) * cols, cols)
        coef_copies.append([
            pltpu.make_async_copy(
                coef.at[pair % nodes, plane, :, pl.ds(column, cols)], blocks.at[pair, plane], coef_sem.at[pair, plane]
            )
            for plane in range(2)
        ])
    for level in range(2):
        for k in range(nodes):
            cw_copies[level, k] = pltpu.make_async_copy(colw.at[level, k], cw.at[level, k], cw_sem.at[level, k])
        for pair in range(pairs):
            node = turned(n, turn_of(pair)) * nodes + pair % nodes
            rw_copies[level, pair] = pltpu.make_async_copy(roww.at[level, node], rw.at[level, pair], rw_sem.at[level, pair])

    for pair in coef_copies:
        for copy in pair:
            copy.start()
    barrier = pltpu.get_barrier_semaphore()
    across = partner[2][0]
    greeted = partner + [(row, turned(n, turn)) for turn in range(1, turns) for row in (w, across)]
    for device in greeted:
        pl.semaphore_signal(barrier, inc=1, device_id=device, device_id_type=MESH)
    for level in range(2):
        for k in range(nodes):
            cw_copies[level, k].start()

    def exchange(stage_index, c, src, dst, device):
        return pltpu.make_async_remote_copy(
            src_ref=src,
            dst_ref=dst,
            send_sem=send.at[stage_index, c],
            recv_sem=recv.at[stage_index, c],
            device_id=device,
            device_id_type=MESH,
        )

    ex1 = [exchange(0, c, x1.at[c, b1], x1.at[c, b1], partner[0]) for c in range(chunks)]
    ex2 = [exchange(1, c, x2.at[c, b2], x2.at[c, b2], partner[1]) for c in range(chunks)]
    relay, ex3 = {}, []
    for c in range(chunks):
        turn = turn_of(c // PARTS)
        owner = turned(n, turn)
        source = stage.at[c] if turn else x3.at[c, b3]
        if turn:
            relay[c] = exchange(2, c, source, x3.at[c, b3], (w, owner))
        ex3.append(exchange(3, c, source, x3.at[c, b3], (across, owner)))
    ex4 = [exchange(4, c, x4.at[c, b4], x4.at[c, b4], partner[3]) for c in range(chunks)]
    out_copies = []

    def prepare(pair):
        for copy in coef_copies[pair]:
            copy.wait()
        parts = traded(blocks[pair, 0].astype(jnp.float32), blocks[pair, 1].astype(jnp.float32))
        for part in range(PARTS):
            x1[pair * PARTS + part, b1] = parts[part].astype(jnp.bfloat16)

    def begin(c):
        if c % PARTS == 0 and c > 0:
            prepare(c // PARTS)
        ex1[c].start()

    prepare(0)
    pl.semaphore_wait(barrier, len(greeted))
    for c in range(AHEAD):
        begin(c)
    for pair in range(pairs):
        for level in range(2):
            rw_copies[level, pair].start()
    for step, c in events(chunks):
        pair, part = c // PARTS, c % PARTS
        k = pair % nodes
        if step == 0:
            if c + AHEAD < chunks:
                begin(c + AHEAD)
            if pair < nodes and part == 0:
                cw_copies[0, k].wait()
            ex1[c].wait_recv()
            x2[c, b2] = product(cw.at[0, k], x1.at[c]).astype(jnp.bfloat16)
            ex2[c].start()
        elif step == 1:
            if pair < nodes and part == 0:
                cw_copies[1, k].wait()
            ex2[c].wait_recv()
            if c in relay:
                stage[c] = product(cw.at[1, k], x2.at[c]).astype(jnp.bfloat16)
                ex3[c].start()
                relay[c].start()
            else:
                x3[c, b3] = product(cw.at[1, k], x2.at[c]).astype(jnp.bfloat16)
                ex3[c].start()
        elif step == 2:
            if part == 0:
                rw_copies[0, pair].wait()
            if c in relay:
                relay[c].wait_recv()
            ex3[c].wait_recv()
            x4[c, b4] = product(rw.at[0, pair], x3.at[c]).astype(jnp.bfloat16)
            ex4[c].start()
        else:
            if part == 0:
                rw_copies[1, pair].wait()
            ex4[c].wait_recv()
            result = product(rw.at[1, pair], x4.at[c])
            if part == 0:
                done[pair, 0] = result.astype(jnp.bfloat16)
            else:
                node = turned(n, turn_of(pair)) * nodes + k
                for plane, value in enumerate(traded(done[pair, 0].astype(jnp.float32), result)):
                    done[pair, plane] = value.astype(jnp.bfloat16)
                copy = pltpu.make_async_copy(done.at[pair], out.at[node], out_sem.at[pair])
                copy.start()
                out_copies.append(copy)
    for copy in ex1 + ex2 + list(relay.values()) + ex3 + ex4:
        copy.wait_send()
    for copy in out_copies:
        copy.wait()


def solution(mesh):
    narrow = mesh.shape["narrow"]
    wide_bits = mesh.shape["wide"].bit_length() - 1

    def per_device(coefficients, col_weights, row_weights):
        nodes, _, rank, count = coefficients.shape
        cols = count // narrow
        pairs = nodes * narrow
        chunks = pairs * PARTS
        block = (chunks, 2, rank, cols)
        dtype = jnp.bfloat16
        flops = 4 * pairs * 2 * 2 * rank * 2 * rank * 2 * cols
        moved = 2 * (coefficients.size * 2 + col_weights.size + row_weights.size)
        dma = pltpu.SemaphoreType.DMA
        return pl.pallas_call(
            functools.partial(kernel, wide_bits),
            out_shape=jax.ShapeDtypeStruct((pairs, 2, rank, cols), dtype),
            in_specs=[pl.BlockSpec(memory_space=pl.ANY)] * 3,
            out_specs=pl.BlockSpec(memory_space=pl.ANY),
            scratch_shapes=[
                pltpu.VMEM((pairs, 2, rank, cols), dtype),
                pltpu.VMEM(block, dtype),
                pltpu.VMEM(block, dtype),
                pltpu.VMEM(block, dtype),
                pltpu.VMEM(block, dtype),
                pltpu.VMEM((chunks, rank, cols), dtype),
                pltpu.VMEM((pairs, 2, rank, cols), dtype),
                pltpu.VMEM((2, nodes, 2, rank, 2 * rank), dtype),
                pltpu.VMEM((2, pairs, 2, rank, 2 * rank), dtype),
                dma((pairs, 2)),
                dma((2, nodes)),
                dma((2, pairs)),
                dma((pairs,)),
                dma((5, chunks)),
                dma((5, chunks)),
            ],
            compiler_params=pltpu.CompilerParams(
                collective_id=0, has_side_effects=True, vmem_limit_bytes=60 * 2**20
            ),
            cost_estimate=pl.CostEstimate(flops=flops, bytes_accessed=moved, transcendentals=0),
        )(coefficients, col_weights, row_weights)

    return jax.shard_map(
        per_device,
        mesh=mesh,
        in_specs=(
            P(("wide", "narrow"), None, None, None),
            P(None, ("wide", "narrow"), None, None, None),
            P(None, "wide", None, None, None),
        ),
        out_specs=P("wide", None, None, "narrow"),
        check_vma=False,
    )
```

```python
import functools

import jax
import jax.numpy as jnp
from jax import lax
from jax.experimental import pallas as pl
from jax.experimental.pallas import tpu as pltpu
from jax.sharding import PartitionSpec as P

MESH = pl.DeviceIdType.MESH
AHEAD = 1
PARTS = 2
LAGS = (2.05, 1.6, 2.6)
VMEM_LIMIT = 52


def turned(index, turn):
    if turn == 0:
        return index
    if turn == 1:
        return index + 1 - 2 * (index % 2)
    if turn == 2:
        return index + 2 - 4 * (index // 2)
    return 3 - index


def halves(width):
    return lax.broadcasted_iota(jnp.int32, (1, width), 1) < width // 2


def crossed(array):
    return pltpu.roll(array, array.shape[1] // 2, 1)


def product(weights, block):
    merged = block[...].reshape(weights.shape[2], block.shape[2])
    first = jnp.dot(weights[0], merged, preferred_element_type=jnp.float32)
    second = crossed(jnp.dot(weights[1], merged, preferred_element_type=jnp.float32))
    return jnp.where(halves(merged.shape[1]), first - second, first + second)


def traded(a, b):
    left = halves(a.shape[1])
    return jnp.where(left, a, crossed(b)), jnp.where(left, crossed(a), b)


def plan(nodes):
    stay = [(turn, k, part) for turn in (0, 1) for k in range(nodes) for part in range(PARTS)]
    leave = [(turn, k, part) for turn in (3, 2) for k in range(nodes) for part in range(PARTS)]
    half = len(stay) // 2
    chunks = []
    for i in range(len(stay)):
        chunks += (stay[i], leave[i]) if i < half else (leave[i], stay[i])
    return chunks


def events(chunks):
    expected = (0, LAGS[0], LAGS[0] + LAGS[1], sum(LAGS))
    return [(level, c) for _, level, c in sorted((c + late, level, c) for c in range(chunks) for level, late in enumerate(expected))]


def kernel(wide_bits, coef, colw, roww, out, blocks, x1, x2, x3, x4, stage, held, cw, rw,
           coef_sem, cw_sem, rw_sem, send, recv):
    w = lax.axis_index("wide")
    n = lax.axis_index("narrow")
    nodes = coef.shape[0]
    order = plan(nodes)
    chunks = len(order)
    pairs = list(dict.fromkeys((turn, k) for turn, k, _ in order))
    pair_of = [pairs.index(chunk[:2]) for chunk in order]
    members = [[c for c in range(chunks) if pair_of[c] == pair] for pair in range(len(pairs))]
    cols = blocks.shape[3]

    def bit(i):
        return (w // 2**i) % 2

    def swapped(i):
        return w + 2**i - 2 ** (i + 1) * bit(i)

    levels = (0, 1, wide_bits - 2, wide_bits - 1)
    b1, b2, b3, b4 = (bit(i) for i in levels)
    partner = [(swapped(i), n) for i in levels]

    coef_copies, rw_copies = [], []
    for pair, (turn, k) in enumerate(pairs):
        owner = turned(n, turn)
        column = pl.multiple_of(owner * cols, cols)
        coef_copies.append(pltpu.make_async_copy(coef.at[k, :, :, pl.ds(column, cols)], blocks.at[pair], coef_sem.at[pair]))
        rw_copies.append(pltpu.make_async_copy(roww.at[:, owner * nodes + k], rw.at[:, pair], rw_sem.at[pair]))
    cw_copies = [pltpu.make_async_copy(colw.at[:, k], cw.at[:, k], cw_sem.at[k]) for k in range(nodes)]

    for copy in coef_copies:
        copy.start()
    barrier = pltpu.get_barrier_semaphore()
    across = partner[2][0]
    greeted = partner + [(row, turned(n, turn)) for turn in (1, 2, 3) for row in (w, across)]
    for device in greeted:
        pl.semaphore_signal(barrier, inc=1, device_id=device, device_id_type=MESH)
    for copy in cw_copies:
        copy.start()

    def exchange(stage_index, c, src, dst, device):
        return pltpu.make_async_remote_copy(
            src_ref=src,
            dst_ref=dst,
            send_sem=send.at[stage_index],
            recv_sem=recv.at[stage_index, c],
            device_id=device,
            device_id_type=MESH,
        )

    ex1 = [exchange(0, c, x1.at[c, b1], x1.at[c, b1], partner[0]) for c in range(chunks)]
    ex2 = [exchange(1, c, x2.at[c, b2], x2.at[c, b2], partner[1]) for c in range(chunks)]
    relay, ex3 = {}, []
    for c, (turn, _, _) in enumerate(order):
        owner = turned(n, turn)
        source = stage.at[c] if turn else x3.at[c, b3]
        if turn:
            relay[c] = exchange(2, c, source, x3.at[c, b3], (w, owner))
        ex3.append(exchange(3, c, source, x3.at[c, b3], (across, owner)))
    ex4 = [exchange(4, c, x4.at[c, b4], x4.at[c, b4], partner[3]) for c in range(chunks)]

    def prepare(pair):
        coef_copies[pair].wait()
        parts = traded(blocks[pair, 0].astype(jnp.float32), blocks[pair, 1].astype(jnp.float32))
        for c, part in zip(members[pair], parts, strict=True):
            x1[c, b1] = part.astype(jnp.bfloat16)

    def begin(c):
        if c == members[pair_of[c]][0] and c > 0:
            prepare(pair_of[c])
        ex1[c].start()

    prepare(0)
    pl.semaphore_wait(barrier, len(greeted))
    for c in range(AHEAD):
        begin(c)
    for copy in rw_copies:
        copy.start()
    unread = {"cw": set(range(nodes)), "rw": set(range(len(pairs)))}

    def loaded(name, i):
        if i in unread[name]:
            unread[name].remove(i)
            (cw_copies if name == "cw" else rw_copies)[i].wait()

    for step, c in events(chunks):
        pair = pair_of[c]
        k = pairs[pair][1]
        if step == 0:
            if c + AHEAD < chunks:
                begin(c + AHEAD)
            loaded("cw", k)
            ex1[c].wait_recv()
            x2[c, b2] = product(cw.at[0, k], x1.at[c]).astype(jnp.bfloat16)
            ex2[c].start()
        elif step == 1:
            ex2[c].wait_recv()
            if c in relay:
                stage[c] = product(cw.at[1, k], x2.at[c]).astype(jnp.bfloat16)
                ex3[c].start()
                relay[c].start()
            else:
                x3[c, b3] = product(cw.at[1, k], x2.at[c]).astype(jnp.bfloat16)
                ex3[c].start()
        elif step == 2:
            loaded("rw", pair)
            if c in relay:
                relay[c].wait_recv()
            ex3[c].wait_recv()
            x4[c, b4] = product(rw.at[0, pair], x3.at[c]).astype(jnp.bfloat16)
            ex4[c].start()
        else:
            ex4[c].wait_recv()
            result = product(rw.at[1, pair], x4.at[c])
            if c == members[pair][0]:
                held[pair] = result.astype(jnp.bfloat16)
            else:
                node = turned(n, pairs[pair][0]) * nodes + k
                for plane, value in enumerate(traded(held[pair].astype(jnp.float32), result)):
                    out[node, plane] = value.astype(jnp.bfloat16)
    for i, (sent, copies) in enumerate(((x1, ex1), (x2, ex2), (stage, relay), (x3, ex3), (x4, ex4))):
        whole = sent if sent is stage else sent.at[:, 0]
        whole = whole.at[pl.ds(0, len(copies))]
        pltpu.make_async_copy(whole, whole, send.at[i]).wait()


def solution(mesh):
    narrow = mesh.shape["narrow"]
    wide_bits = mesh.shape["wide"].bit_length() - 1

    def per_device(coefficients, col_weights, row_weights):
        nodes, _, rank, count = coefficients.shape
        cols = count // narrow
        pairs = nodes * narrow
        chunks = pairs * PARTS
        block = (chunks, 2, rank, cols)
        dtype = jnp.bfloat16
        flops = 4 * pairs * 2 * 2 * rank * 2 * rank * 2 * cols
        moved = 2 * (coefficients.size * 2 + col_weights.size + row_weights.size)
        dma = pltpu.SemaphoreType.DMA
        return pl.pallas_call(
            functools.partial(kernel, wide_bits),
            out_shape=jax.ShapeDtypeStruct((pairs, 2, rank, cols), dtype),
            in_specs=[pl.BlockSpec(memory_space=pl.ANY)] * 3,
            out_specs=pl.BlockSpec(memory_space=pltpu.VMEM),
            scratch_shapes=[
                pltpu.VMEM((pairs, 2, rank, cols), dtype),
                pltpu.VMEM(block, dtype),
                pltpu.VMEM(block, dtype),
                pltpu.VMEM(block, dtype),
                pltpu.VMEM(block, dtype),
                pltpu.VMEM((chunks, rank, cols), dtype),
                pltpu.VMEM((pairs, rank, cols), dtype),
                pltpu.VMEM((2, nodes, 2, rank, 2 * rank), dtype),
                pltpu.VMEM((2, pairs, 2, rank, 2 * rank), dtype),
                dma((pairs,)),
                dma((nodes,)),
                dma((pairs,)),
                dma((5,)),
                dma((5, chunks)),
            ],
            compiler_params=pltpu.CompilerParams(
                collective_id=0, has_side_effects=True, vmem_limit_bytes=VMEM_LIMIT * 2**20
            ),
            cost_estimate=pl.CostEstimate(flops=flops, bytes_accessed=moved, transcendentals=0),
        )(coefficients, col_weights, row_weights)

    return jax.shard_map(
        per_device,
        mesh=mesh,
        in_specs=(
            P(("wide", "narrow"), None, None, None),
            P(None, ("wide", "narrow"), None, None, None),
            P(None, "wide", None, None, None),
        ),
        out_specs=P("wide", None, None, "narrow"),
        check_vma=False,
    )
```

```python
import functools

import jax
import jax.numpy as jnp
from jax import lax
from jax.experimental import pallas as pl
from jax.experimental.pallas import tpu as pltpu
from jax.sharding import PartitionSpec as P

MESH = pl.DeviceIdType.MESH
AHEAD = 2
SLOTS = 8
PARTS = 2
LAGS = (2.05, 1.6, 2.6)
VMEM_LIMIT = 52


def turned(index, turn):
    if turn == 0:
        return index
    if turn == 1:
        return index + 1 - 2 * (index % 2)
    if turn == 2:
        return index + 2 - 4 * (index // 2)
    return 3 - index


def halves(width):
    return lax.broadcasted_iota(jnp.int32, (1, width), 1) < width // 2


def crossed(array):
    return pltpu.roll(array, array.shape[1] // 2, 1)


def product(weights, block):
    merged = block[...].reshape(weights.shape[2], block.shape[2])
    first = jnp.dot(weights[0], merged, preferred_element_type=jnp.float32)
    second = crossed(jnp.dot(weights[1], merged, preferred_element_type=jnp.float32))
    return jnp.where(halves(merged.shape[1]), first - second, first + second)


def traded(a, b):
    left = halves(a.shape[1])
    return jnp.where(left, a, crossed(b)), jnp.where(left, crossed(a), b)


def plan(nodes):
    stay = [(turn, k, part) for turn in (0, 1) for k in range(nodes) for part in range(PARTS)]
    leave = [(turn, k, part) for turn in (3, 2) for k in range(nodes) for part in range(PARTS)]
    half = len(stay) // 2
    chunks = []
    for i in range(len(stay)):
        chunks += (stay[i], leave[i]) if i < half else (leave[i], stay[i])
    return chunks


def events(chunks):
    expected = (0, LAGS[0], LAGS[0] + LAGS[1], sum(LAGS))
    return [(level, c) for _, level, c in sorted((c + late, level, c) for c in range(chunks) for level, late in enumerate(expected))]


def kernel(wide_bits, coef, colw, roww, out, blocks, x1, x2, x3, x4, stage, held, cw, rw,
           coef_sem, cw_sem, rw_sem, send, recv):
    w = lax.axis_index("wide")
    n = lax.axis_index("narrow")
    nodes = coef.shape[0]
    order = plan(nodes)
    chunks = len(order)
    pairs = list(dict.fromkeys((turn, k) for turn, k, _ in order))
    pair_of = [pairs.index(chunk[:2]) for chunk in order]
    members = [[c for c in range(chunks) if pair_of[c] == pair] for pair in range(len(pairs))]
    cols = blocks.shape[3]

    def bit(i):
        return (w // 2**i) % 2

    def swapped(i):
        return w + 2**i - 2 ** (i + 1) * bit(i)

    levels = (0, 1, wide_bits - 2, wide_bits - 1)
    b1, b2, b3, b4 = (bit(i) for i in levels)
    partner = [(swapped(i), n) for i in levels]

    coef_copies, rw_copies = [], []
    for pair, (turn, k) in enumerate(pairs):
        owner = turned(n, turn)
        column = pl.multiple_of(owner * cols, cols)
        coef_copies.append(pltpu.make_async_copy(coef.at[k, :, :, pl.ds(column, cols)], blocks.at[pair], coef_sem.at[pair]))
        rw_copies.append(pltpu.make_async_copy(roww.at[:, owner * nodes + k], rw.at[:, pair], rw_sem.at[pair]))
    cw_copies = [pltpu.make_async_copy(colw.at[:, k], cw.at[:, k], cw_sem.at[k]) for k in range(nodes)]

    for copy in coef_copies:
        copy.start()
    barrier = pltpu.get_barrier_semaphore()
    across = partner[2][0]
    greeted = partner + [(row, turned(n, turn)) for turn in (1, 2, 3) for row in (w, across)]
    for device in greeted:
        pl.semaphore_signal(barrier, inc=1, device_id=device, device_id_type=MESH)
    for copy in cw_copies:
        copy.start()

    def landed(stage_index, c):
        if stage_index in (2, 3):
            return recv.at[3 * SLOTS + (stage_index - 2) * chunks + c]
        return recv.at[(0, 1, None, None, 2)[stage_index] * SLOTS + c % SLOTS]

    def exchange(stage_index, c, src, dst, device):
        return pltpu.make_async_remote_copy(
            src_ref=src,
            dst_ref=dst,
            send_sem=send.at[stage_index],
            recv_sem=landed(stage_index, c),
            device_id=device,
            device_id_type=MESH,
        )

    ex1 = [exchange(0, c, x1.at[c, b1], x1.at[c, b1], partner[0]) for c in range(chunks)]
    ex2 = [exchange(1, c, x2.at[c, b2], x2.at[c, b2], partner[1]) for c in range(chunks)]
    relay, ex3 = {}, []
    for c, (turn, _, _) in enumerate(order):
        owner = turned(n, turn)
        source = stage.at[c] if turn else x3.at[c, b3]
        if turn:
            relay[c] = exchange(2, c, source, x3.at[c, b3], (w, owner))
        ex3.append(exchange(3, c, source, x3.at[c, b3], (across, owner)))
    ex4 = [exchange(4, c, x4.at[c, b4], x4.at[c, b4], partner[3]) for c in range(chunks)]

    def prepare(pair):
        coef_copies[pair].wait()
        parts = traded(blocks[pair, 0].astype(jnp.float32), blocks[pair, 1].astype(jnp.float32))
        for c, part in zip(members[pair], parts, strict=True):
            x1[c, b1] = part.astype(jnp.bfloat16)

    def begin(c):
        if c == members[pair_of[c]][0] and c > 0:
            prepare(pair_of[c])
        ex1[c].start()

    prepare(0)
    pl.semaphore_wait(barrier, len(greeted))
    for c in range(AHEAD):
        begin(c)
    for copy in rw_copies:
        copy.start()
    unread = {"cw": set(range(nodes)), "rw": set(range(len(pairs)))}

    def loaded(name, i):
        if i in unread[name]:
            unread[name].remove(i)
            (cw_copies if name == "cw" else rw_copies)[i].wait()

    for step, c in events(chunks):
        pair = pair_of[c]
        k = pairs[pair][1]
        if step == 0:
            if c + AHEAD < chunks:
                begin(c + AHEAD)
            loaded("cw", k)
            ex1[c].wait_recv()
            x2[c, b2] = product(cw.at[0, k], x1.at[c]).astype(jnp.bfloat16)
            ex2[c].start()
        elif step == 1:
            ex2[c].wait_recv()
            if c in relay:
                stage[c] = product(cw.at[1, k], x2.at[c]).astype(jnp.bfloat16)
                ex3[c].start()
                relay[c].start()
            else:
                x3[c, b3] = product(cw.at[1, k], x2.at[c]).astype(jnp.bfloat16)
                ex3[c].start()
        elif step == 2:
            loaded("rw", pair)
            if c in relay:
                relay[c].wait_recv()
            ex3[c].wait_recv()
            x4[c, b4] = product(rw.at[0, pair], x3.at[c]).astype(jnp.bfloat16)
            ex4[c].start()
        else:
            ex4[c].wait_recv()
            result = product(rw.at[1, pair], x4.at[c])
            if c == members[pair][0]:
                held[pair] = result.astype(jnp.bfloat16)
            else:
                node = turned(n, pairs[pair][0]) * nodes + k
                for plane, value in enumerate(traded(held[pair].astype(jnp.float32), result)):
                    out[node, plane] = value.astype(jnp.bfloat16)
    for i, (sent, copies) in enumerate(((x1, ex1), (x2, ex2), (stage, relay), (x3, ex3), (x4, ex4))):
        whole = sent if sent is stage else sent.at[:, 0]
        whole = whole.at[pl.ds(0, len(copies))]
        pltpu.make_async_copy(whole, whole, send.at[i]).wait()


def solution(mesh):
    narrow = mesh.shape["narrow"]
    wide_bits = mesh.shape["wide"].bit_length() - 1

    def per_device(coefficients, col_weights, row_weights):
        nodes, _, rank, count = coefficients.shape
        cols = count // narrow
        pairs = nodes * narrow
        chunks = pairs * PARTS
        block = (chunks, 2, rank, cols)
        dtype = jnp.bfloat16
        flops = 4 * pairs * 2 * 2 * rank * 2 * rank * 2 * cols
        moved = 2 * (coefficients.size * 2 + col_weights.size + row_weights.size)
        dma = pltpu.SemaphoreType.DMA
        return pl.pallas_call(
            functools.partial(kernel, wide_bits),
            out_shape=jax.ShapeDtypeStruct((pairs, 2, rank, cols), dtype),
            in_specs=[pl.BlockSpec(memory_space=pl.ANY)] * 3,
            out_specs=pl.BlockSpec(memory_space=pltpu.VMEM),
            scratch_shapes=[
                pltpu.VMEM((pairs, 2, rank, cols), dtype),
                pltpu.VMEM(block, dtype),
                pltpu.VMEM(block, dtype),
                pltpu.VMEM(block, dtype),
                pltpu.VMEM(block, dtype),
                pltpu.VMEM((chunks, rank, cols), dtype),
                pltpu.VMEM((pairs, rank, cols), dtype),
                pltpu.VMEM((2, nodes, 2, rank, 2 * rank), dtype),
                pltpu.VMEM((2, pairs, 2, rank, 2 * rank), dtype),
                dma((pairs,)),
                dma((nodes,)),
                dma((pairs,)),
                dma((5,)),
                dma((3 * SLOTS + 2 * chunks,)),
            ],
            compiler_params=pltpu.CompilerParams(
                collective_id=0, has_side_effects=True, vmem_limit_bytes=VMEM_LIMIT * 2**20
            ),
            cost_estimate=pl.CostEstimate(flops=flops, bytes_accessed=moved, transcendentals=0),
        )(coefficients, col_weights, row_weights)

    return jax.shard_map(
        per_device,
        mesh=mesh,
        in_specs=(
            P(("wide", "narrow"), None, None, None),
            P(None, ("wide", "narrow"), None, None, None),
            P(None, "wide", None, None, None),
        ),
        out_specs=P("wide", None, None, "narrow"),
        check_vma=False,
    )
```
